256 devices in a mesh: rep: 8 (over x, z_lo), blk: 32 (over z_hi, y, core).
Axes of the slice: x: 4, y: 4, z: 8 (z_hi: 4, z_lo: 2; z = z_hi * 2 + z_lo), core: 2. Of those that a mesh axis runs over, the one named last changes fastest.
Arguments:
- positions: float32 [3, 65536], P(None, ('rep', 'blk')), parts along dimension 1, may hold values from 0 to 64
- forces: float32 [6, 3, 65536], P(None, None, ('rep', 'blk')), parts along dimension 2, may hold values from -6 to 6
- random_kicks: float32 [6, 3, 65536], P(None, None, ('rep', 'blk')), parts along dimension 2, may hold values from -4 to 4
- history_velocity: float32 [128, 3, 65536], P(None, None, ('rep', 'blk')), parts along dimension 2, may hold values from -6 to 6
- history_offset: float32 [128, 3, 65536], P(None, None, ('rep', 'blk')), parts along dimension 2, may hold values from -8 to 8
- lag_index: int32 [32768], P(('rep', 'blk')), parts along dimension 0, may hold values from 0 to 127
Outputs:
- final_positions: float32 [3, 65536], P(None, ('rep', 'blk')), parts along dimension 1
- velocity: float32 [3, 65536], P(None, ('rep', 'blk')), parts along dimension 1
- statistics: float32 [2, 32768], P(None, ('rep', 'blk')), parts along dimension 1
The draws below stay inside these ranges and needn't reach their ends.
There are 8 independent parts, one for each index of `rep`. The reference program is written for one: setup_inputs(seed, part) draws one part's arguments, and reference() takes and returns one part's arrays. A program takes and returns all parts, laid end to end along the dimension named above; each array names one. Nothing has to cross between parts.
All inputs are finite; a program needn't handle non-finite values.
Results may differ from the reference program's by a relative error of at most 0.0003.
Values sent between devices are 32-bit elements; how exact they have to be, the bound alone decides.
No kernel may reach another device: no remote copies, remote signals or barrier semaphores. Data moves between devices by JAX's collectives and lax.ppermute only.
A program may use at most 64 MiB of HBM per device.

```python
import math
import jax
import jax.numpy as jnp
from jax import lax

STEPS = 6
HIST = 128
SPHERES = 8192
NLAG = 4096


def plant(result, own_key, least, high):
    longest = result.shape.index(max(result.shape))
    spots = []
    for shift in (0, 1):
        where = [jax.random.randint(jax.random.fold_in(own_key, axis), (), 0, length) for axis, length in enumerate(result.shape)]
        where[longest] = (where[longest] + shift) % result.shape[longest]
        spots.append(tuple(where))
    return result.at[spots[0]].set(least).at[spots[1]].set(high)


def steps_of(key, dims, pieces, least, high):
    factor_of, own = 1.0, jax.random.fold_in(key, 6)
    for axis_at, parts in pieces:
        draws = jnp.exp(jax.random.uniform(jax.random.fold_in(own, axis_at), (parts,), jnp.float32, least / len(pieces), high / len(pieces)))
        factor_of = factor_of * jnp.repeat(draws, dims[axis_at] // parts).reshape([-1 if axis == axis_at else 1 for axis in range(len(dims))])
    return factor_of


def noise(own_key, shape, spread, most, pieces=(), kind=jnp.bfloat16):
    array = spread * jax.random.normal(own_key, shape, jnp.float32)
    if pieces:
        array = array * steps_of(own_key, shape, pieces, -0.22, 0.18)
    return jnp.clip(array, -most, most).astype(kind)


def setup_inputs(seed: int = 0, part: int = 0) -> dict:
    arg_keys = jax.random.split(jax.random.key(seed), 7)
    own_keys = jax.random.split(jax.random.fold_in(arg_keys[6], part), 7)
    positions = jnp.clip(64.0 * jax.random.uniform(own_keys[0], (3, SPHERES), jnp.float32) ** steps_of(own_keys[0], (3, SPHERES), ((1, 32),), -0.2, 0.2), 0.0, 64.0)
    forces = noise(own_keys[1], (STEPS, 3, SPHERES), 1.0, 6.0, ((2, 32),), jnp.float32)
    random_kicks = noise(own_keys[2], (STEPS, 3, SPHERES), 0.3, 4.0, ((2, 32),), jnp.float32)
    history_velocity = noise(own_keys[3], (HIST, 3, SPHERES), 1.0, 6.0, ((2, 32),), jnp.float32)
    history_offset = noise(own_keys[4], (HIST, 3, SPHERES), 2.0, 8.0, ((2, 32),), jnp.float32)
    lag_index = plant(jax.random.randint(own_keys[5], (NLAG,), 0, HIST), jax.random.fold_in(own_keys[5], 1), 0, HIST - 1).astype(jnp.int32)
    return dict(positions=positions, forces=forces, random_kicks=random_kicks, history_velocity=history_velocity, history_offset=history_offset, lag_index=lag_index)


time_step = 0.05

def pair_velocity(targets, sources, loads):
    separation = targets[:, None, :] - sources[:, :, None]
    dist_sq = lax.optimization_barrier(jnp.sum(separation * separation, axis=0))
    dist_safe = jnp.where(dist_sq > 0.0, dist_sq, 1.0)
    inv_dist = lax.rsqrt(dist_safe)
    distance = dist_sq * inv_dist
    inv_sq = 1.0 / dist_safe
    far_mask = distance >= 2.0
    coef_iso = jnp.where(far_mask, 0.75 * inv_dist * (1.0 + 2.0 / 3.0 * inv_sq), 1.0 - 9.0 / 32.0 * distance)
    coef_dir = jnp.where(far_mask, 0.75 * inv_dist * (1.0 - 2.0 * inv_sq) * inv_sq, 3.0 / 32.0 * inv_dist)
    projection = lax.optimization_barrier(jnp.sum(separation * loads[:, :, None], axis=0))
    return lax.optimization_barrier(jnp.sum(coef_iso[None] * loads[:, :, None] + (coef_dir * projection)[None] * separation, axis=1))

def velocities(places, loads):
    row_count = math.gcd(SPHERES, 512)
    block_count = SPHERES // row_count
    source_blocks = places.reshape(3, block_count, row_count).transpose(1, 0, 2)
    load_blocks = loads.reshape(3, block_count, row_count).transpose(1, 0, 2)

    def accumulate(running, source_block):
        return (running + pair_velocity(places, source_block[0], source_block[1]), None)
    running, unused = lax.scan(accumulate, jnp.zeros((3, SPHERES), jnp.float32), (source_blocks, load_blocks))
    return running

def reference(positions, forces, random_kicks, history_velocity, history_offset, lag_index):
    places = positions
    velocity = jnp.zeros_like(positions)
    for step_index in range(STEPS):
        velocity = velocities(places, forces[step_index])
        places = places + time_step * velocity + random_kicks[step_index]
    velocity_dot = lax.optimization_barrier(jnp.sum(velocity[None] * history_velocity, axis=(1, 2)))
    moved = places[None] - positions[None] - history_offset
    square_disp = lax.optimization_barrier(jnp.sum(moved * moved, axis=(1, 2)))
    statistics = jnp.stack([velocity_dot[lag_index], square_disp[lag_index]]) / jnp.float32(SPHERES)
    return (places, velocity, statistics)
```

```python
import jax
import jax.numpy as jnp
from jax import lax
from jax.experimental import pallas as pl
from jax.experimental.pallas import tpu as pltpu
from jax.sharding import PartitionSpec as P

STEPS = 6
BLK = 256
KROWS = 64
PAIR = 2
CHUNK = 32
BF = jnp.bfloat16
F32 = jnp.float32

time_step = 0.05
CENTRE = 32.0
SIGMA = 0.75**0.5
ROOT3 = 3.0**0.5
ALPHA = 9.0 / (32.0 * SIGMA)
BETA = 1.125 * SIGMA


def halves(a):
    hi = a.astype(BF).astype(F32)
    return hi, a - hi


def thirds(a):
    hi, rest = halves(a)
    mid, low = halves(rest)
    return hi, mid, low


def split_place(x):
    scaled = (x - CENTRE) * SIGMA
    hi = (jnp.round(scaled * 8.0) * 0.125).astype(BF).astype(F32)
    mid = (scaled - hi).astype(BF).astype(F32)
    return hi, mid


def feature_rows(hi, mid):
    hh = hi[0] * hi[0] + hi[1] * hi[1] + hi[2] * hi[2]
    hm = 2.0 * (hi[0] * mid[0] + hi[1] * mid[1] + hi[2] * mid[2])
    mm = mid[0] * mid[0] + mid[1] * mid[1] + mid[2] * mid[2]
    return thirds(hh), thirds(hm), halves(mm)


def source_table(x, f):
    hi, mid = zip(*(split_place(a) for a in x))
    fh = [a.astype(BF).astype(F32) for a in f]
    fm = [(a - b).astype(BF).astype(F32) for a, b in zip(f, fh)]
    hh, hm, mm = feature_rows(hi, mid)
    along = thirds(sum((h + m) * (a + b) for h, m, a, b in zip(hi, mid, fh, fm)))
    one, zero = jnp.ones_like(hi[0]), jnp.zeros_like(hi[0])
    minus_hi = [-2.0 * a for a in hi]
    minus_mid = [-2.0 * a for a in mid]
    rows = [*minus_hi, *hh, one, one, one] + [zero] * 7
    rows += [*minus_hi, *minus_mid, *hm, one, one, one] + [zero] * 4
    rows += [*minus_mid, *mm, one, one, zero]
    rows += [*fh, *fm, *fh, *fm, *along] + [zero] * 9
    weights = [*fh, *fm, *hi, *mid, one, zero, zero, zero]
    return rows, weights


def target_table(hi, mid):
    h, m = [hi[c : c + 1] for c in range(3)], [mid[c : c + 1] for c in range(3)]
    hh, hm, mm = feature_rows(h, m)
    one, zero = jnp.ones_like(h[0]), jnp.zeros_like(h[0])
    dist = [*h, one, one, one, *hh] + [zero] * 7
    dist += [*m, *h, one, one, one, *hm] + [zero] * 4
    dist += [*m, one, one, *mm, zero] + [zero] * 24
    proj = [zero] * 40 + [*h, *h, *m, *m, -one, -one, -one] + [zero] * 9
    return jnp.concatenate(
        [jnp.concatenate(dist, axis=0), jnp.concatenate(proj, axis=0)], axis=1
    ).astype(BF)


def pair_kernel(blocks, xs_ref, fs_ref, own_ref, kick_ref, place_ref, vel_ref, rows_ref, weights_ref,
                even_ref, odd_ref, even_coef_ref, odd_coef_ref):
    def spread(ref, groups_of_8, group, k, row):
        at = ((group // 8) * groups_of_8 + k // 8) * 64 + k % 8
        for half in range(2):
            ref[half, pl.ds(at, 8, stride=8), :] = row[:, half * 128 : half * 128 + 128]

    for group in range(0, blocks, 8):
        part = pl.ds(group, 8)
        x = [xs_ref[part, c * BLK : (c + 1) * BLK] for c in range(3)]
        f = [fs_ref[part, c * BLK : (c + 1) * BLK] for c in range(3)]
        rows, weights = source_table(x, f)
        for k, row in enumerate(rows):
            spread(rows_ref, KROWS // 8, group, k, row)
        for k, row in enumerate(weights):
            spread(weights_ref, 2, group, k, row)

    own = own_ref[...]
    hi, mid = split_place(own)
    table = target_table(hi, mid)

    def block_rows(ref, groups_of_8, b, half):
        at = ((b // 8) * groups_of_8 * 8 + b % 8) * 8
        return jnp.concatenate(
            [ref[half, pl.ds(pl.multiple_of(at + g * 64, 8), 8), :] for g in range(groups_of_8)], axis=0
        ).astype(BF)

    def geometry(b0, both_ref):
        lhs = jnp.concatenate(
            [block_rows(rows_ref, KROWS // 8, b0 + n, h).T for n in range(PAIR) for h in range(2)], axis=0
        )
        both_ref[...] = jnp.dot(lhs, table, preferred_element_type=F32)

    def coefficients(both_ref, coef_ref):
        for at in range(0, PAIR * BLK, CHUNK):
            rows = slice(at, at + CHUNK)
            dist_sq = jnp.maximum(both_ref[rows, :BLK], 1e-8)
            along = both_ref[rows, BLK:]
            inv = lax.rsqrt(dist_sq)
            inv_far = jnp.minimum(inv, 1.0 / ROOT3)
            inv_sq = inv_far * inv_far
            iso = inv_far * (2.0 + inv_sq) + jnp.maximum(ROOT3 - dist_sq * inv, 0.0)
            pull = inv * (inv_sq * (2.0 / 3.0 - inv_sq)) * along
            iso_hi = iso.astype(BF)
            pull_hi = pull.astype(BF)
            coef_ref[0, rows, :] = iso_hi
            coef_ref[1, rows, :] = (iso - iso_hi.astype(F32)).astype(BF)
            coef_ref[2, rows, :] = pull_hi
            coef_ref[3, rows, :] = (pull - pull_hi.astype(F32)).astype(BF)

    def totals(b0, coef_ref, sums):
        w = jnp.concatenate(
            [block_rows(weights_ref, 2, b0 + n, h) for n in range(PAIR) for h in range(2)], axis=1
        )
        dot = lambda a: jnp.dot(w, a, preferred_element_type=F32)
        return (
            sums[0] + (dot(coef_ref[0]) + dot(coef_ref[1])),
            sums[1] + (dot(coef_ref[2]) + dot(coef_ref[3])),
        )

    def trip(i, sums):
        b0 = i * (2 * PAIR)
        geometry(b0 + PAIR, odd_ref)
        coefficients(even_ref, even_coef_ref)
        sums = totals(jnp.maximum(b0 - PAIR, 0), odd_coef_ref, sums)
        geometry(jnp.minimum(b0 + 2 * PAIR, blocks - PAIR), even_ref)
        coefficients(odd_ref, odd_coef_ref)
        sums = totals(b0, even_coef_ref, sums)
        return sums

    nothing = jnp.zeros((16, BLK), F32)
    odd_coef_ref[...] = jnp.zeros_like(odd_coef_ref)
    geometry(0, even_ref)
    sums = lax.fori_loop(0, blocks // (2 * PAIR), trip, (nothing, nothing))
    iso_sum, pull_sum = totals(blocks - PAIR, odd_coef_ref, sums)
    vel = ALPHA * (iso_sum[0:3] + iso_sum[3:6]) + BETA * (
        (hi + mid) * pull_sum[12:13] - (pull_sum[6:9] + pull_sum[9:12])
    )
    vel_ref[...] = vel
    place_ref[...] = own + time_step * vel + kick_ref[...]


def pair_step(xs, fs, own, kick):
    blocks = xs.shape[0]
    vmem = pl.BlockSpec(memory_space=pltpu.VMEM)
    out = jax.ShapeDtypeStruct(own.shape, F32)
    return pl.pallas_call(
        lambda *refs: pair_kernel(blocks, *refs),
        out_shape=(out, out),
        in_specs=[vmem] * 4,
        out_specs=(vmem, vmem),
        scratch_shapes=[
            pltpu.VMEM((2, blocks * KROWS, 128), F32),
            pltpu.VMEM((2, blocks * 16, 128), F32),
            pltpu.VMEM((PAIR * BLK, 2 * BLK), F32),
            pltpu.VMEM((PAIR * BLK, 2 * BLK), F32),
            pltpu.VMEM((4, PAIR * BLK, BLK), BF),
            pltpu.VMEM((4, PAIR * BLK, BLK), BF),
        ],
        cost_estimate=pl.CostEstimate(flops=10**8, bytes_accessed=10**6, transcendentals=0),
        compiler_params=pltpu.CompilerParams(vmem_limit_bytes=40 * 2**20),
        name="pair_step",
    )(xs, fs, own, kick)


def sent_to_all(x, axis):
    copies = jnp.broadcast_to(x, (lax.axis_size(axis), *x.shape))
    return lax.all_to_all(copies, axis, split_axis=0, concat_axis=0, tiled=True)


def local(positions, forces, random_kicks, history_velocity, history_offset, lag_index):
    places = positions
    width = 3 * BLK
    first = jnp.concatenate([positions.reshape(-1), forces.reshape(-1)])
    everything = sent_to_all(first, "blk")
    blocks = everything.shape[0]
    for step in range(STEPS):
        if step == 0:
            xs = everything[:, :width]
        else:
            xs = sent_to_all(places.reshape(-1), "blk")
        fs = everything[:, (step + 1) * width : (step + 2) * width]
        places, velocity = pair_step(xs, fs, places, random_kicks[step])
    velocity_dot = jnp.sum(velocity[None] * history_velocity, axis=(1, 2))
    moved = places[None] - positions[None] - history_offset
    square_disp = jnp.sum(moved * moved, axis=(1, 2))
    frames = history_velocity.shape[0]
    sphere_total = jnp.float32(positions.shape[1] * blocks)
    sums = jnp.sum(sent_to_all(jnp.concatenate([velocity_dot, square_disp]), "blk"), axis=0)
    frame_table = jnp.stack([sums[:frames], sums[frames:]], axis=1)
    onehot = (lag_index[:, None] == jnp.arange(frames, dtype=jnp.int32)[None, :]).astype(F32)
    picked = jnp.dot(onehot, frame_table, precision=lax.Precision.HIGHEST, preferred_element_type=F32)
    statistics = picked.T / sphere_total
    return (places, velocity, statistics)


def solution(mesh):
    return jax.shard_map(
        local,
        mesh=mesh,
        in_specs=(
            P(None, ("rep", "blk")),
            P(None, None, ("rep", "blk")),
            P(None, None, ("rep", "blk")),
            P(None, None, ("rep", "blk")),
            P(None, None, ("rep", "blk")),
            P(("rep", "blk")),
        ),
        out_specs=(P(None, ("rep", "blk")), P(None, ("rep", "blk")), P(None, ("rep", "blk"))),
        check_vma=False,
    )
```

```python
import jax
import jax.numpy as jnp
from jax import lax
from jax.experimental import pallas as pl
from jax.experimental.pallas import tpu as pltpu
from jax.sharding import PartitionSpec as P

STEPS = 6
BLK = 256
KROWS = 64
UNROLL = 16
CHUNK = 128
AHEAD = 3
BF = jnp.bfloat16
F32 = jnp.float32

time_step = 0.05
CENTRE = 32.0
SIGMA = 0.75**0.5
ROOT3 = 3.0**0.5
ALPHA = 9.0 / (32.0 * SIGMA)
BETA = 1.125 * SIGMA


def halves(a):
    hi = a.astype(BF).astype(F32)
    return hi, a - hi


def thirds(a):
    hi, rest = halves(a)
    mid, low = halves(rest)
    return hi, mid, low


def split_place(x):
    scaled = (x - CENTRE) * SIGMA
    hi = (jnp.round(scaled * 8.0) * 0.125).astype(BF).astype(F32)
    mid = (scaled - hi).astype(BF).astype(F32)
    return hi, mid


def feature_rows(hi, mid):
    hh = hi[0] * hi[0] + hi[1] * hi[1] + hi[2] * hi[2]
    hm = 2.0 * (hi[0] * mid[0] + hi[1] * mid[1] + hi[2] * mid[2])
    mm = mid[0] * mid[0] + mid[1] * mid[1] + mid[2] * mid[2]
    return thirds(hh), thirds(hm), halves(mm)


def source_table(x, f):
    hi, mid = zip(*(split_place(a) for a in x))
    fh = [a.astype(BF).astype(F32) for a in f]
    fm = [(a - b).astype(BF).astype(F32) for a, b in zip(f, fh)]
    hh, hm, mm = feature_rows(hi, mid)
    along = thirds(sum((h + m) * (a + b) for h, m, a, b in zip(hi, mid, fh, fm)))
    one, zero = jnp.ones_like(hi[0]), jnp.zeros_like(hi[0])
    minus_hi = [-2.0 * a for a in hi]
    minus_mid = [-2.0 * a for a in mid]
    rows = [*minus_hi, *hh, one, one, one] + [zero] * 7
    rows += [*minus_hi, *minus_mid, *hm, one, one, one] + [zero] * 4
    rows += [*minus_mid, *mm, one, one, zero]
    rows += [*fh, *fm, *fh, *fm, *along] + [zero] * 9
    weights = [*fh, *fm, *hi, *mid, one, zero, zero, zero]
    return rows, weights


def target_table(hi, mid):
    h, m = [hi[c : c + 1] for c in range(3)], [mid[c : c + 1] for c in range(3)]
    hh, hm, mm = feature_rows(h, m)
    one, zero = jnp.ones_like(h[0]), jnp.zeros_like(h[0])
    dist = [*h, one, one, one, *hh] + [zero] * 7
    dist += [*m, *h, one, one, one, *hm] + [zero] * 4
    dist += [*m, one, one, *mm, zero] + [zero] * 24
    proj = [zero] * 40 + [*h, *h, *m, *m, -one, -one, -one] + [zero] * 9
    return jnp.concatenate(
        [jnp.concatenate(dist, axis=0), jnp.concatenate(proj, axis=0)], axis=1
    ).astype(BF)


def pair_kernel(blocks, xs_ref, fs_ref, own_ref, kick_ref, place_ref, vel_ref, rows_ref, weights_ref):
    def spread(ref, groups_of_8, group, k, row):
        at = ((group // 8) * groups_of_8 + k // 8) * 64 + k % 8
        for half in range(2):
            ref[half, pl.ds(at, 8, stride=8), :] = row[:, half * 128 : half * 128 + 128]

    for group in range(0, blocks, 8):
        part = pl.ds(group, 8)
        x = [xs_ref[part, c * BLK : (c + 1) * BLK] for c in range(3)]
        f = [fs_ref[part, c * BLK : (c + 1) * BLK] for c in range(3)]
        rows, weights = source_table(x, f)
        for k, row in enumerate(rows):
            spread(rows_ref, KROWS // 8, group, k, row)
        for k, row in enumerate(weights):
            spread(weights_ref, 2, group, k, row)

    own = own_ref[...]
    hi, mid = split_place(own)
    table = target_table(hi, mid)

    def block_rows(ref, groups_of_8, b, half):
        at = ((b // 8) * groups_of_8 * 8 + b % 8) * 8
        return jnp.concatenate(
            [ref[half, pl.ds(pl.multiple_of(at + g * 64, 8), 8), :] for g in range(groups_of_8)], axis=0
        ).astype(BF)

    def source_columns(b):
        return jnp.concatenate([block_rows(rows_ref, KROWS // 8, b, h).T for h in range(2)], axis=0)

    def geometry(columns):
        return jnp.dot(columns, table, preferred_element_type=F32)

    def coefficients(both):
        dist_sq = jnp.maximum(both[:, :BLK], 1e-8)
        along = both[:, BLK:]
        inv = lax.rsqrt(dist_sq)
        inv_far = jnp.minimum(inv, 1.0 / ROOT3)
        inv_sq = inv_far * inv_far
        iso = inv_far * (2.0 + inv_sq) + jnp.maximum(ROOT3 - dist_sq * inv, 0.0)
        pull = inv * (inv_sq * (2.0 / 3.0 - inv_sq)) * along
        iso_hi = iso.astype(BF)
        pull_hi = pull.astype(BF)
        iso_lo = (iso - iso_hi.astype(F32)).astype(BF)
        pull_lo = (pull - pull_hi.astype(F32)).astype(BF)
        return iso_hi, iso_lo, pull_hi, pull_lo

    def weight_rows(b):
        return jnp.concatenate([block_rows(weights_ref, 2, b, h) for h in range(2)], axis=1)

    def trip(i, sums):
        iso_sum, pull_sum = sums
        b0 = i * UNROLL
        pieces = BLK // CHUNK
        columns = [source_columns(b0 + n) for n in range(UNROLL)]
        at = lambda c: columns[c // pieces][(c % pieces) * CHUNK : (c % pieces + 1) * CHUNK]
        ahead = [geometry(at(c)) for c in range(AHEAD)]
        for c in range(UNROLL * pieces):
            if c + AHEAD < UNROLL * pieces:
                ahead.append(geometry(at(c + AHEAD)))
            if c % pieces == 0:
                w = weight_rows(b0 + c // pieces)
            iso_hi, iso_lo, pull_hi, pull_lo = coefficients(ahead.pop(0))
            piece = w[:, (c % pieces) * CHUNK : (c % pieces + 1) * CHUNK]
            dot = lambda a: jnp.dot(piece, a, preferred_element_type=F32)
            iso_sum = iso_sum + (dot(iso_hi) + dot(iso_lo))
            pull_sum = pull_sum + (dot(pull_hi) + dot(pull_lo))
        return iso_sum, pull_sum

    nothing = jnp.zeros((16, BLK), F32)
    iso_sum, pull_sum = lax.fori_loop(0, blocks // UNROLL, trip, (nothing, nothing))
    vel = ALPHA * (iso_sum[0:3] + iso_sum[3:6]) + BETA * (
        (hi + mid) * pull_sum[12:13] - (pull_sum[6:9] + pull_sum[9:12])
    )
    vel_ref[...] = vel
    place_ref[...] = own + time_step * vel + kick_ref[...]


def pair_step(xs, fs, own, kick):
    blocks = xs.shape[0]
    vmem = pl.BlockSpec(memory_space=pltpu.VMEM)
    out = jax.ShapeDtypeStruct(own.shape, F32)
    return pl.pallas_call(
        lambda *refs: pair_kernel(blocks, *refs),
        out_shape=(out, out),
        in_specs=[vmem] * 4,
        out_specs=(vmem, vmem),
        scratch_shapes=[
            pltpu.VMEM((2, blocks * KROWS, 128), F32),
            pltpu.VMEM((2, blocks * 16, 128), F32),
        ],
        cost_estimate=pl.CostEstimate(flops=10**8, bytes_accessed=10**6, transcendentals=0),
        compiler_params=pltpu.CompilerParams(vmem_limit_bytes=40 * 2**20),
        name="pair_step",
    )(xs, fs, own, kick)


def sent_to_all(x, axis):
    copies = jnp.broadcast_to(x, (lax.axis_size(axis), *x.shape))
    return lax.all_to_all(copies, axis, split_axis=0, concat_axis=0, tiled=True)


def local(positions, forces, random_kicks, history_velocity, history_offset, lag_index):
    places = positions
    width = 3 * BLK
    first = jnp.concatenate([positions.reshape(-1), forces.reshape(-1)])
    everything = sent_to_all(first, "blk")
    blocks = everything.shape[0]
    for step in range(STEPS):
        if step == 0:
            xs = everything[:, :width]
        else:
            xs = sent_to_all(places.reshape(-1), "blk")
        fs = everything[:, (step + 1) * width : (step + 2) * width]
        places, velocity = pair_step(xs, fs, places, random_kicks[step])
    velocity_dot = jnp.sum(velocity[None] * history_velocity, axis=(1, 2))
    moved = places[None] - positions[None] - history_offset
    square_disp = jnp.sum(moved * moved, axis=(1, 2))
    frames = history_velocity.shape[0]
    sphere_total = jnp.float32(positions.shape[1] * blocks)
    sums = jnp.sum(sent_to_all(jnp.concatenate([velocity_dot, square_disp]), "blk"), axis=0)
    frame_table = jnp.stack([sums[:frames], sums[frames:]], axis=1)
    onehot = (lag_index[:, None] == jnp.arange(frames, dtype=jnp.int32)[None, :]).astype(F32)
    picked = jnp.dot(onehot, frame_table, precision=lax.Precision.HIGHEST, preferred_element_type=F32)
    statistics = picked.T / sphere_total
    return (places, velocity, statistics)


def solution(mesh):
    return jax.shard_map(
        local,
        mesh=mesh,
        in_specs=(
            P(None, ("rep", "blk")),
            P(None, None, ("rep", "blk")),
            P(None, None, ("rep", "blk")),
            P(None, None, ("rep", "blk")),
            P(None, None, ("rep", "blk")),
            P(("rep", "blk")),
        ),
        out_specs=(P(None, ("rep", "blk")), P(None, ("rep", "blk")), P(None, ("rep", "blk"))),
        check_vma=False,
    )
```

```python
import jax
import jax.numpy as jnp
from jax import lax
from jax.experimental import pallas as pl
from jax.experimental.pallas import tpu as pltpu
from jax.sharding import PartitionSpec as P

STEPS = 6
BLK = 256
KROWS = 64
UNROLL = 16
CHUNK = 64
AHEAD = 5
BF = jnp.bfloat16
F32 = jnp.float32

time_step = 0.05
CENTRE = 32.0
SIGMA = 0.75**0.5
ROOT3 = 3.0**0.5
ALPHA = 9.0 / (32.0 * SIGMA)
BETA = 1.125 * SIGMA


def halves(a):
    hi = a.astype(BF).astype(F32)
    return hi, a - hi


def thirds(a):
    hi, rest = halves(a)
    mid, low = halves(rest)
    return hi, mid, low


def split_place(x):
    scaled = (x - CENTRE) * SIGMA
    hi = (jnp.round(scaled * 8.0) * 0.125).astype(BF).astype(F32)
    mid = (scaled - hi).astype(BF).astype(F32)
    return hi, mid


def feature_rows(hi, mid):
    hh = hi[0] * hi[0] + hi[1] * hi[1] + hi[2] * hi[2]
    hm = 2.0 * (hi[0] * mid[0] + hi[1] * mid[1] + hi[2] * mid[2])
    mm = mid[0] * mid[0] + mid[1] * mid[1] + mid[2] * mid[2]
    return thirds(hh), thirds(hm), halves(mm)


def source_table(x, f):
    hi, mid = zip(*(split_place(a) for a in x))
    fh = [a.astype(BF).astype(F32) for a in f]
    fm = [(a - b).astype(BF).astype(F32) for a, b in zip(f, fh)]
    hh, hm, mm = feature_rows(hi, mid)
    along = thirds(sum((h + m) * (a + b) for h, m, a, b in zip(hi, mid, fh, fm)))
    one, zero = jnp.ones_like(hi[0]), jnp.zeros_like(hi[0])
    minus_hi = [-2.0 * a for a in hi]
    minus_mid = [-2.0 * a for a in mid]
    rows = [*minus_hi, *hh, one, one, one] + [zero] * 7
    rows += [*minus_hi, *minus_mid, *hm, one, one, one] + [zero] * 4
    rows += [*minus_mid, *mm, one, one, zero]
    rows += [*fh, *fm, *fh, *fm, *along] + [zero] * 9
    weights = [*fh, *fm, *hi, *mid, one, zero, zero, zero]
    return rows, weights


def target_table(hi, mid):
    h, m = [hi[c : c + 1] for c in range(3)], [mid[c : c + 1] for c in range(3)]
    hh, hm, mm = feature_rows(h, m)
    one, zero = jnp.ones_like(h[0]), jnp.zeros_like(h[0])
    dist = [*h, one, one, one, *hh] + [zero] * 7
    dist += [*m, *h, one, one, one, *hm] + [zero] * 4
    dist += [*m, one, one, *mm, zero] + [zero] * 24
    proj = [zero] * 40 + [*h, *h, *m, *m, -one, -one, -one] + [zero] * 9
    return jnp.concatenate(
        [jnp.concatenate(dist, axis=0), jnp.concatenate(proj, axis=0)], axis=1
    ).astype(BF)


def pair_kernel(blocks, xs_ref, fs_ref, own_ref, kick_ref, place_ref, vel_ref, rows_ref, weights_ref):
    def spread(ref, groups_of_8, group, k, row):
        at = ((group // 8) * groups_of_8 + k // 8) * 64 + k % 8
        for half in range(2):
            ref[half, pl.ds(at, 8, stride=8), :] = row[:, half * 128 : half * 128 + 128]

    for group in range(0, blocks, 8):
        part = pl.ds(group, 8)
        x = [xs_ref[part, c * BLK : (c + 1) * BLK] for c in range(3)]
        f = [fs_ref[part, c * BLK : (c + 1) * BLK] for c in range(3)]
        rows, weights = source_table(x, f)
        for k, row in enumerate(rows):
            spread(rows_ref, KROWS // 8, group, k, row)
        for k, row in enumerate(weights):
            spread(weights_ref, 2, group, k, row)

    own = own_ref[...]
    hi, mid = split_place(own)
    table = target_table(hi, mid)

    def block_rows(ref, groups_of_8, b, half):
        at = ((b // 8) * groups_of_8 * 8 + b % 8) * 8
        return jnp.concatenate(
            [ref[half, pl.ds(pl.multiple_of(at + g * 64, 8), 8), :] for g in range(groups_of_8)], axis=0
        ).astype(BF)

    def source_columns(b):
        return jnp.concatenate([block_rows(rows_ref, KROWS // 8, b, h).T for h in range(2)], axis=0)

    def geometry(columns):
        return jnp.dot(columns, table, preferred_element_type=F32)

    def coefficients(both):
        dist_sq = both[:, :BLK]
        along = both[:, BLK:]
        inv = lax.rsqrt(jnp.maximum(dist_sq, 1e-8))
        inv_far = jnp.minimum(inv, 1.0 / ROOT3)
        inv_sq = inv_far * inv_far
        iso = inv_far * (2.0 + inv_sq) + jnp.maximum(ROOT3 - dist_sq * inv, 0.0)
        pull = inv * (inv_sq * (2.0 / 3.0 - inv_sq)) * along
        iso_hi = iso.astype(BF)
        pull_hi = pull.astype(BF)
        iso_lo = (iso - iso_hi.astype(F32)).astype(BF)
        pull_lo = (pull - pull_hi.astype(F32)).astype(BF)
        return iso_hi, iso_lo, pull_hi, pull_lo

    def weight_rows(b):
        return jnp.concatenate([block_rows(weights_ref, 2, b, h) for h in range(2)], axis=1)

    def trip(i, sums):
        iso_sum, pull_sum = sums
        b0 = i * UNROLL
        pieces = BLK // CHUNK
        columns = [source_columns(b0 + n) for n in range(UNROLL)]
        at = lambda c: columns[c // pieces][(c % pieces) * CHUNK : (c % pieces + 1) * CHUNK]
        ahead = [geometry(at(c)) for c in range(AHEAD)]
        for c in range(UNROLL * pieces):
            if c + AHEAD < UNROLL * pieces:
                ahead.append(geometry(at(c + AHEAD)))
            if c % pieces == 0:
                w = weight_rows(b0 + c // pieces)
            iso_hi, iso_lo, pull_hi, pull_lo = coefficients(ahead.pop(0))
            piece = w[:, (c % pieces) * CHUNK : (c % pieces + 1) * CHUNK]
            twice = jnp.concatenate([piece, piece], axis=1)
            dot = lambda *a: jnp.dot(twice, jnp.concatenate(a, axis=0), preferred_element_type=F32)
            iso_sum = iso_sum + dot(iso_hi, iso_lo)
            pull_sum = pull_sum + dot(pull_hi, pull_lo)
        return iso_sum, pull_sum

    nothing = jnp.zeros((16, BLK), F32)
    iso_sum, pull_sum = lax.fori_loop(0, blocks // UNROLL, trip, (nothing, nothing))
    vel = ALPHA * (iso_sum[0:3] + iso_sum[3:6]) + BETA * (
        (hi + mid) * pull_sum[12:13] - (pull_sum[6:9] + pull_sum[9:12])
    )
    vel_ref[...] = vel
    place_ref[...] = own + time_step * vel + kick_ref[...]


def pair_step(xs, fs, own, kick):
    blocks = xs.shape[0]
    vmem = pl.BlockSpec(memory_space=pltpu.VMEM)
    out = jax.ShapeDtypeStruct(own.shape, F32)
    return pl.pallas_call(
        lambda *refs: pair_kernel(blocks, *refs),
        out_shape=(out, out),
        in_specs=[vmem] * 4,
        out_specs=(vmem, vmem),
        scratch_shapes=[
            pltpu.VMEM((2, blocks * KROWS, 128), F32),
            pltpu.VMEM((2, blocks * 16, 128), F32),
        ],
        cost_estimate=pl.CostEstimate(flops=10**8, bytes_accessed=10**6, transcendentals=0),
        compiler_params=pltpu.CompilerParams(vmem_limit_bytes=40 * 2**20),
        name="pair_step",
    )(xs, fs, own, kick)


def sent_to_all(x, axis):
    copies = jnp.broadcast_to(x, (lax.axis_size(axis), *x.shape))
    return lax.all_to_all(copies, axis, split_axis=0, concat_axis=0, tiled=True)


def local(positions, forces, random_kicks, history_velocity, history_offset, lag_index):
    places = positions
    width = 3 * BLK
    first = jnp.concatenate([positions.reshape(-1), forces.reshape(-1)])
    everything = sent_to_all(first, "blk")
    blocks = everything.shape[0]
    for step in range(STEPS):
        if step == 0:
            xs = everything[:, :width]
        else:
            xs = sent_to_all(places.reshape(-1), "blk")
        fs = everything[:, (step + 1) * width : (step + 2) * width]
        places, velocity = pair_step(xs, fs, places, random_kicks[step])
    velocity_dot = jnp.sum(velocity[None] * history_velocity, axis=(1, 2))
    moved = places[None] - positions[None] - history_offset
    square_disp = jnp.sum(moved * moved, axis=(1, 2))
    frames = history_velocity.shape[0]
    sphere_total = jnp.float32(positions.shape[1] * blocks)
    sums = jnp.sum(sent_to_all(jnp.concatenate([velocity_dot, square_disp]), "blk"), axis=0)
    frame_table = jnp.stack([sums[:frames], sums[frames:]], axis=1)
    onehot = (lag_index[:, None] == jnp.arange(frames, dtype=jnp.int32)[None, :]).astype(F32)
    picked = jnp.dot(onehot, frame_table, precision=lax.Precision.HIGHEST, preferred_element_type=F32)
    statistics = picked.T / sphere_total
    return (places, velocity, statistics)


def solution(mesh):
    return jax.shard_map(
        local,
        mesh=mesh,
        in_specs=(
            P(None, ("rep", "blk")),
            P(None, None, ("rep", "blk")),
            P(None, None, ("rep", "blk")),
            P(None, None, ("rep", "blk")),
            P(None, None, ("rep", "blk")),
            P(("rep", "blk")),
        ),
        out_specs=(P(None, ("rep", "blk")), P(None, ("rep", "blk")), P(None, ("rep", "blk"))),
        check_vma=False,
    )
```

```python
import jax
import jax.numpy as jnp
from jax import lax
from jax.experimental import pallas as pl
from jax.experimental.pallas import tpu as pltpu
from jax.sharding import PartitionSpec as P

STEPS = 6
BLK = 256
KROWS = 64
UNROLL = 16
CHUNK = 64
AHEAD = 5
BF = jnp.bfloat16
F32 = jnp.float32

time_step = 0.05
CENTRE = 32.0
SIGMA = 0.75**0.5
ROOT3 = 3.0**0.5
ALPHA = 9.0 / (32.0 * SIGMA)
BETA = 1.125 * SIGMA


def halves(a):
    hi = a.astype(BF).astype(F32)
    return hi, a - hi


def thirds(a):
    hi, rest = halves(a)
    mid, low = halves(rest)
    return hi, mid, low


def split_place(x):
    scaled = (x - CENTRE) * SIGMA
    hi = (jnp.round(scaled * 8.0) * 0.125).astype(BF).astype(F32)
    mid = (scaled - hi).astype(BF).astype(F32)
    return hi, mid


def feature_rows(hi, mid):
    hh = hi[0] * hi[0] + hi[1] * hi[1] + hi[2] * hi[2]
    hm = 2.0 * (hi[0] * mid[0] + hi[1] * mid[1] + hi[2] * mid[2])
    mm = mid[0] * mid[0] + mid[1] * mid[1] + mid[2] * mid[2]
    return thirds(hh), thirds(hm), halves(mm)


def source_table(x, f):
    hi, mid = zip(*(split_place(a) for a in x))
    fh = [a.astype(BF).astype(F32) for a in f]
    fm = [(a - b).astype(BF).astype(F32) for a, b in zip(f, fh)]
    hh, hm, mm = feature_rows(hi, mid)
    along = thirds(sum((h + m) * (a + b) for h, m, a, b in zip(hi, mid, fh, fm)))
    one, zero = jnp.ones_like(hi[0]), jnp.zeros_like(hi[0])
    minus_hi = [-2.0 * a for a in hi]
    minus_mid = [-2.0 * a for a in mid]
    rows = [*minus_hi, *hh, one, one, one] + [zero] * 7
    rows += [*minus_hi, *minus_mid, *hm, one, one, one] + [zero] * 4
    rows += [*minus_mid, *mm, one, one, zero]
    rows += [*fh, *fm, *fh, *fm, *along] + [zero] * 9
    weights = [*fh, *fm, *hi, *mid, one, zero, zero, zero]
    return rows, weights


def target_table(hi, mid):
    h, m = [hi[c : c + 1] for c in range(3)], [mid[c : c + 1] for c in range(3)]
    hh, hm, mm = feature_rows(h, m)
    one, zero = jnp.ones_like(h[0]), jnp.zeros_like(h[0])
    dist = [*h, one, one, one, *hh] + [zero] * 7
    dist += [*m, *h, one, one, one, *hm] + [zero] * 4
    dist += [*m, one, one, *mm, zero] + [zero] * 24
    proj = [zero] * 40 + [*h, *h, *m, *m, -one, -one, -one] + [zero] * 9
    return jnp.concatenate(
        [jnp.concatenate(dist, axis=0), jnp.concatenate(proj, axis=0)], axis=1
    ).astype(BF)


def pair_kernel(blocks, xs_ref, fs_ref, own_ref, kick_ref, place_ref, vel_ref, rows_ref, weights_ref):
    def spread(ref, groups_of_8, group, k, row):
        at = ((group // 8) * groups_of_8 + k // 8) * 64 + k % 8
        for half in range(2):
            ref[half, pl.ds(at, 8, stride=8), :] = row[:, half * 128 : half * 128 + 128]

    for group in range(0, blocks, 8):
        part = pl.ds(group, 8)
        x = [xs_ref[part, c * BLK : (c + 1) * BLK] for c in range(3)]
        f = [fs_ref[part, c * BLK : (c + 1) * BLK] for c in range(3)]
        rows, weights = source_table(x, f)
        for k, row in enumerate(rows):
            spread(rows_ref, KROWS // 8, group, k, row)
        for k, row in enumerate(weights):
            spread(weights_ref, 2, group, k, row)

    own = own_ref[...]
    hi, mid = split_place(own)
    table = target_table(hi, mid)

    def block_rows(ref, groups_of_8, b, half):
        at = ((b // 8) * groups_of_8 * 8 + b % 8) * 8
        return jnp.concatenate(
            [ref[half, pl.ds(pl.multiple_of(at + g * 64, 8), 8), :] for g in range(groups_of_8)], axis=0
        ).astype(BF)

    def source_columns(b):
        return jnp.concatenate([block_rows(rows_ref, KROWS // 8, b, h).T for h in range(2)], axis=0)

    def geometry(columns):
        return jnp.dot(columns, table, preferred_element_type=F32)

    def coefficients(both):
        dist_sq = jnp.maximum(both[:, :BLK], 1e-8)
        along = both[:, BLK:]
        inv = lax.rsqrt(dist_sq)
        inv_far = jnp.minimum(inv, 1.0 / ROOT3)
        inv_sq = inv_far * inv_far
        iso = inv_far * (2.0 + inv_sq) + jnp.maximum(ROOT3 - dist_sq * inv, 0.0)
        pull = inv * (inv_sq * (2.0 / 3.0 - inv_sq)) * along
        iso_hi = iso.astype(BF)
        pull_hi = pull.astype(BF)
        iso_lo = (iso - iso_hi.astype(F32)).astype(BF)
        pull_lo = (pull - pull_hi.astype(F32)).astype(BF)
        return iso_hi, iso_lo, pull_hi, pull_lo

    def weight_rows(b):
        return jnp.concatenate([block_rows(weights_ref, 2, b, h) for h in range(2)], axis=1)

    def trip(i, sums):
        iso_sum, pull_sum = sums
        b0 = i * UNROLL
        pieces = BLK // CHUNK
        columns = [source_columns(b0 + n) for n in range(UNROLL)]
        at = lambda c: columns[c // pieces][(c % pieces) * CHUNK : (c % pieces + 1) * CHUNK]
        ahead = [geometry(at(c)) for c in range(AHEAD)]
        for c in range(UNROLL * pieces):
            if c + AHEAD < UNROLL * pieces:
                ahead.append(geometry(at(c + AHEAD)))
            if c % pieces == 0:
                w = weight_rows(b0 + c // pieces)
            iso_hi, iso_lo, pull_hi, pull_lo = coefficients(ahead.pop(0))
            piece = w[:, (c % pieces) * CHUNK : (c % pieces + 1) * CHUNK]
            twice = jnp.concatenate([piece, piece], axis=1)
            dot = lambda *a: jnp.dot(twice, jnp.concatenate(a, axis=0), preferred_element_type=F32)
            iso_sum = iso_sum + dot(iso_hi, iso_lo)
            pull_sum = pull_sum + dot(pull_hi, pull_lo)
        return iso_sum, pull_sum

    nothing = jnp.zeros((16, BLK), F32)
    iso_sum, pull_sum = lax.fori_loop(0, blocks // UNROLL, trip, (nothing, nothing))
    vel = ALPHA * (iso_sum[0:3] + iso_sum[3:6]) + BETA * (
        (hi + mid) * pull_sum[12:13] - (pull_sum[6:9] + pull_sum[9:12])
    )
    vel_ref[...] = vel
    place_ref[...] = own + time_step * vel + kick_ref[...]


def pair_step(xs, fs, own, kick):
    blocks = xs.shape[0]
    vmem = pl.BlockSpec(memory_space=pltpu.VMEM)
    out = jax.ShapeDtypeStruct(own.shape, F32)
    return pl.pallas_call(
        lambda *refs: pair_kernel(blocks, *refs),
        out_shape=(out, out),
        in_specs=[vmem] * 4,
        out_specs=(vmem, vmem),
        scratch_shapes=[
            pltpu.VMEM((2, blocks * KROWS, 128), F32),
            pltpu.VMEM((2, blocks * 16, 128), F32),
        ],
        cost_estimate=pl.CostEstimate(flops=10**8, bytes_accessed=10**6, transcendentals=0),
        compiler_params=pltpu.CompilerParams(vmem_limit_bytes=40 * 2**20),
        name="pair_step",
    )(xs, fs, own, kick)


def sent_to_all(x, axis):
    copies = jnp.broadcast_to(x, (lax.axis_size(axis), *x.shape))
    return lax.all_to_all(copies, axis, split_axis=0, concat_axis=0, tiled=True)


def local(positions, forces, random_kicks, history_velocity, history_offset, lag_index):
    places = positions
    width = 3 * BLK
    first = jnp.concatenate([positions.reshape(-1), forces.reshape(-1)])
    everything = sent_to_all(first, "blk")
    blocks = everything.shape[0]
    for step in range(STEPS):
        if step == 0:
            xs = everything[:, :width]
        else:
            xs = sent_to_all(places.reshape(-1), "blk")
        fs = everything[:, (step + 1) * width : (step + 2) * width]
        places, velocity = pair_step(xs, fs, places, random_kicks[step])
    velocity_dot = jnp.sum(velocity[None] * history_velocity, axis=(1, 2))
    moved = places[None] - positions[None] - history_offset
    square_disp = jnp.sum(moved * moved, axis=(1, 2))
    frames = history_velocity.shape[0]
    sphere_total = jnp.float32(positions.shape[1] * blocks)
    sums = jnp.sum(sent_to_all(jnp.concatenate([velocity_dot, square_disp]), "blk"), axis=0)
    frame_table = jnp.stack([sums[:frames], sums[frames:]], axis=1)
    onehot = (lag_index[:, None] == jnp.arange(frames, dtype=jnp.int32)[None, :]).astype(F32)
    picked = jnp.dot(onehot, frame_table, precision=lax.Precision.HIGHEST, preferred_element_type=F32)
    statistics = picked.T / sphere_total
    return (places, velocity, statistics)


def solution(mesh):
    return jax.shard_map(
        local,
        mesh=mesh,
        in_specs=(
            P(None, ("rep", "blk")),
            P(None, None, ("rep", "blk")),
            P(None, None, ("rep", "blk")),
            P(None, None, ("rep", "blk")),
            P(None, None, ("rep", "blk")),
            P(("rep", "blk")),
        ),
        out_specs=(P(None, ("rep", "blk")), P(None, ("rep", "blk")), P(None, ("rep", "blk"))),
        check_vma=False,
    )
```

```python
import jax
import jax.numpy as jnp
from jax import lax
from jax.experimental import pallas as pl
from jax.experimental.pallas import tpu as pltpu
from jax.sharding import PartitionSpec as P

STEPS = 6
BLK = 256
KROWS = 64
UNROLL = 16
CHUNK = 64
AHEAD = 5
BF = jnp.bfloat16
F32 = jnp.float32

time_step = 0.05
CENTRE = 32.0
SIGMA = 0.75**0.5
ROOT3 = 3.0**0.5
ALPHA = 9.0 / (32.0 * SIGMA)
BETA = 1.125 * SIGMA


def halves(a):
    hi = a.astype(BF).astype(F32)
    return hi, a - hi


def thirds(a):
    hi, rest = halves(a)
    mid, low = halves(rest)
    return hi, mid, low


def split_place(x):
    scaled = (x - CENTRE) * SIGMA
    hi = (jnp.round(scaled * 8.0) * 0.125).astype(BF).astype(F32)
    mid = (scaled - hi).astype(BF).astype(F32)
    return hi, mid


def feature_rows(hi, mid):
    hh = hi[0] * hi[0] + hi[1] * hi[1] + hi[2] * hi[2]
    hm = 2.0 * (hi[0] * mid[0] + hi[1] * mid[1] + hi[2] * mid[2])
    mm = mid[0] * mid[0] + mid[1] * mid[1] + mid[2] * mid[2]
    return thirds(hh), thirds(hm), halves(mm)


def source_table(x, f):
    hi, mid = zip(*(split_place(a) for a in x))
    fh = [a.astype(BF).astype(F32) for a in f]
    fm = [(a - b).astype(BF).astype(F32) for a, b in zip(f, fh)]
    hh, hm, mm = feature_rows(hi, mid)
    along = thirds(sum((h + m) * (a + b) for h, m, a, b in zip(hi, mid, fh, fm)))
    one, zero = jnp.ones_like(hi[0]), jnp.zeros_like(hi[0])
    minus_hi = [-2.0 * a for a in hi]
    minus_mid = [-2.0 * a for a in mid]
    rows = [*minus_hi, *hh, one, one, one] + [zero] * 7
    rows += [*minus_hi, *minus_mid, *hm, one, one, one] + [zero] * 4
    rows += [*minus_mid, *mm, one, one, zero]
    rows += [*fh, *fm, *fh, *fm, *along] + [zero] * 9
    weights = [*fh, *fm, *hi, *mid, one, zero, zero, zero]
    return rows, weights


def target_table(hi, mid):
    h, m = [hi[c : c + 1] for c in range(3)], [mid[c : c + 1] for c in range(3)]
    hh, hm, mm = feature_rows(h, m)
    one, zero = jnp.ones_like(h[0]), jnp.zeros_like(h[0])
    dist = [*h, one, one, one, *hh] + [zero] * 7
    dist += [*m, *h, one, one, one, *hm] + [zero] * 4
    dist += [*m, one, one, *mm, zero] + [zero] * 24
    proj = [zero] * 40 + [*h, *h, *m, *m, -one, -one, -one] + [zero] * 9
    return jnp.concatenate(
        [jnp.concatenate(dist, axis=0), jnp.concatenate(proj, axis=0)], axis=1
    ).astype(BF)


def pair_kernel(blocks, xs_ref, fs_ref, own_ref, kick_ref, place_ref, vel_ref, rows_ref, weights_ref):
    def spread(ref, groups_of_8, group, k, row):
        at = ((group // 8) * groups_of_8 + k // 8) * 64 + k % 8
        for half in range(2):
            ref[half, pl.ds(at, 8, stride=8), :] = row[:, half * 128 : half * 128 + 128]

    for group in range(0, blocks, 8):
        part = pl.ds(group, 8)
        x = [xs_ref[part, c * BLK : (c + 1) * BLK] for c in range(3)]
        f = [fs_ref[part, c * BLK : (c + 1) * BLK] for c in range(3)]
        rows, weights = source_table(x, f)
        for k, row in enumerate(rows):
            spread(rows_ref, KROWS // 8, group, k, row)
        for k, row in enumerate(weights):
            spread(weights_ref, 2, group, k, row)

    own = own_ref[...]
    hi, mid = split_place(own)
    table = target_table(hi, mid)

    def block_rows(ref, groups_of_8, b, half):
        at = ((b // 8) * groups_of_8 * 8 + b % 8) * 8
        return jnp.concatenate(
            [ref[half, pl.ds(pl.multiple_of(at + g * 64, 8), 8), :] for g in range(groups_of_8)], axis=0
        ).astype(BF)

    def source_columns(b):
        return jnp.concatenate([block_rows(rows_ref, KROWS // 8, b, h).T for h in range(2)], axis=0)

    def geometry(columns):
        return jnp.dot(columns, table, preferred_element_type=F32)

    def coefficients(both):
        dist_sq = jnp.maximum(both[:, :BLK], 1e-8)
        along = both[:, BLK:]
        inv = lax.rsqrt(dist_sq)
        inv_far = jnp.minimum(inv, 1.0 / ROOT3)
        inv_sq = inv_far * inv_far
        iso = inv_far * (2.0 + inv_sq) + jnp.maximum(ROOT3 - dist_sq * inv, 0.0)
        pull = inv * (inv_sq * (2.0 / 3.0 - inv_sq)) * along
        iso_hi = iso.astype(BF)
        pull_hi = pull.astype(BF)
        iso_lo = (iso - iso_hi.astype(F32)).astype(BF)
        pull_lo = (pull - pull_hi.astype(F32)).astype(BF)
        return iso_hi, iso_lo, pull_hi, pull_lo

    def weight_rows(b):
        return jnp.concatenate([block_rows(weights_ref, 2, b, h) for h in range(2)], axis=1)

    def trip(i, sums):
        iso_sum, pull_sum = sums
        b0 = i * UNROLL
        pieces = BLK // CHUNK
        columns = [source_columns(b0 + n) for n in range(UNROLL)]
        at = lambda c: columns[c // pieces][(c % pieces) * CHUNK : (c % pieces + 1) * CHUNK]
        ahead = [geometry(at(c)) for c in range(AHEAD)]
        for c in range(UNROLL * pieces):
            if c + AHEAD < UNROLL * pieces:
                ahead.append(geometry(at(c + AHEAD)))
            if c % pieces == 0:
                w = weight_rows(b0 + c // pieces)
            iso_hi, iso_lo, pull_hi, pull_lo = coefficients(ahead.pop(0))
            piece = w[:, (c % pieces) * CHUNK : (c % pieces + 1) * CHUNK]
            twice = jnp.concatenate([piece, piece], axis=1)
            dot = lambda *a: jnp.dot(twice, jnp.concatenate(a, axis=0), preferred_element_type=F32)
            iso_sum = iso_sum + dot(iso_hi, iso_lo)
            pull_sum = pull_sum + dot(pull_hi, pull_lo)
        return iso_sum, pull_sum

    nothing = jnp.zeros((16, BLK), F32)
    iso_sum, pull_sum = lax.fori_loop(0, blocks // UNROLL, trip, (nothing, nothing))
    vel = ALPHA * (iso_sum[0:3] + iso_sum[3:6]) + BETA * (
        (hi + mid) * pull_sum[12:13] - (pull_sum[6:9] + pull_sum[9:12])
    )
    vel_ref[...] = vel
    place_ref[...] = own + time_step * vel + kick_ref[...]


def pair_step(xs, fs, own, kick):
    blocks = xs.shape[0]
    vmem = pl.BlockSpec(memory_space=pltpu.VMEM)
    out = jax.ShapeDtypeStruct(own.shape, F32)
    return pl.pallas_call(
        lambda *refs: pair_kernel(blocks, *refs),
        out_shape=(out, out),
        in_specs=[vmem] * 4,
        out_specs=(vmem, vmem),
        scratch_shapes=[
            pltpu.VMEM((2, blocks * KROWS, 128), F32),
            pltpu.VMEM((2, blocks * 16, 128), F32),
        ],
        cost_estimate=pl.CostEstimate(flops=10**8, bytes_accessed=10**6, transcendentals=0),
        compiler_params=pltpu.CompilerParams(vmem_limit_bytes=40 * 2**20),
        name="pair_step",
    )(xs, fs, own, kick)


def sent_to_all(x, axis):
    copies = jnp.broadcast_to(x, (lax.axis_size(axis), *x.shape))
    return lax.all_to_all(copies, axis, split_axis=0, concat_axis=0, tiled=True)


def sent_by_side(x, axis):
    size = lax.axis_size(axis)
    sides = [list(range(side, size, 2)) for side in range(2)]
    copies = jnp.broadcast_to(x, (size // 2, *x.shape))
    own = lax.all_to_all(copies, axis, split_axis=0, concat_axis=0, axis_index_groups=sides, tiled=True)
    other = lax.ppermute(own, axis, [(i, i ^ 1) for i in range(size)])
    even = lax.axis_index(axis) % 2 == 0
    pair = jnp.stack([jnp.where(even, own, other), jnp.where(even, other, own)], axis=1)
    return pair.reshape(size, *x.shape)


def local(positions, forces, random_kicks, history_velocity, history_offset, lag_index):
    places = positions
    width = 3 * BLK
    first = jnp.concatenate([positions.reshape(-1), forces.reshape(-1)])
    everything = sent_by_side(first, "blk")
    blocks = everything.shape[0]
    for step in range(STEPS):
        if step == 0:
            xs = everything[:, :width]
        else:
            xs = sent_to_all(places.reshape(-1), "blk")
        fs = everything[:, (step + 1) * width : (step + 2) * width]
        places, velocity = pair_step(xs, fs, places, random_kicks[step])
    velocity_dot = jnp.sum(velocity[None] * history_velocity, axis=(1, 2))
    moved = places[None] - positions[None] - history_offset
    square_disp = jnp.sum(moved * moved, axis=(1, 2))
    frames = history_velocity.shape[0]
    sphere_total = jnp.float32(positions.shape[1] * blocks)
    sums = jnp.sum(sent_to_all(jnp.concatenate([velocity_dot, square_disp]), "blk"), axis=0)
    frame_table = jnp.stack([sums[:frames], sums[frames:]], axis=1)
    onehot = (lag_index[:, None] == jnp.arange(frames, dtype=jnp.int32)[None, :]).astype(F32)
    picked = jnp.dot(onehot, frame_table, precision=lax.Precision.HIGHEST, preferred_element_type=F32)
    statistics = picked.T / sphere_total
    return (places, velocity, statistics)


def solution(mesh):
    return jax.shard_map(
        local,
        mesh=mesh,
        in_specs=(
            P(None, ("rep", "blk")),
            P(None, None, ("rep", "blk")),
            P(None, None, ("rep", "blk")),
            P(None, None, ("rep", "blk")),
            P(None, None, ("rep", "blk")),
            P(("rep", "blk")),
        ),
        out_specs=(P(None, ("rep", "blk")), P(None, ("rep", "blk")), P(None, ("rep", "blk"))),
        check_vma=False,
    )
```
